32 devices in a mesh: walk: 4 (over y, x), orb: 8 (over z, core).
Axes of the slice: x: 2, y: 2, z: 4, core: 2. Of those that a mesh axis runs over, the one named last changes fastest.
Arguments:
- coefficients: bfloat16 [4096, 4096], P(None, 'orb'), may hold values from -6 to 6
- inverse: bfloat16 [4, 1024, 1024], P('walk', 'orb'), may hold values from -0.005859375 to 0.005859375
- cell_index: int32 [4, 3, 1024], P('walk'), may hold values from 0 to 15
- fraction: float32 [4, 3, 1024], P('walk'), may hold values from 0 to 1
- energies: float32 [4], P('walk'), may hold values from -8 to 8
- weights: float32 [4], P('walk'), may hold values from 0.5 to 2
- occupied: int32 [1024], replicated, may hold values from 0 to 4095, as said below
Outputs:
- gradient: float32 [1024, 4096], P('walk', 'orb')
The draws below stay inside these ranges and needn't reach their ends.
Inputs may be any that keep to these rules, and one draw needn't show every extreme that they name: `occupied`: 1024 distinct orbital indices; every block of 512 consecutive orbital indices holds at most 192 of them, and some block holds exactly 192.
All inputs are finite; a program needn't handle non-finite values.
Results may differ from the reference program's by a relative error of at most 0.019.
Values may be sent and summed in bfloat16 or wider, within the bound.
A program may use at most 64 MiB of HBM per device.

```python
import math
import jax
import jax.numpy as jnp
from jax import lax

N = 1024
M = 4096
GRID = 16
SAMPLES = 4
CELLS = 4096
N_ORB = 8


def draw_occupied(key, part):
    shards = N_ORB
    local = M // N_ORB
    bound = 3 * N // (2 * N_ORB)
    others = shards - 1
    remainder = N - bound
    base = remainder // others
    extra = remainder - base * others
    key_moves = jax.random.fold_in(key, 11)
    key_spot = jax.random.fold_in(key, 12)
    key_score = jax.random.fold_in(key, 13)
    key_order = jax.random.fold_in(key, 14)
    counts = base + (jnp.arange(others, dtype=jnp.int32) < extra).astype(jnp.int32)
    margin = max(0, min(base - 1, bound - base - 2))
    pairs = others // 2
    moves = jax.random.randint(key_moves, (pairs,), 0, margin + 1).astype(jnp.int32)
    change = jnp.zeros((others,), jnp.int32)
    change = change.at[0:2 * pairs:2].add(moves)
    change = change.at[1:2 * pairs:2].add(-moves)
    counts = counts + change
    full = jnp.concatenate([jnp.full((1,), bound, jnp.int32), counts])
    spot = jax.random.randint(key_spot, (), 0, shards)
    full = jnp.roll(full, spot)
    scores = jax.random.randint(key_score, (shards, local), 0, 1 << 20).astype(jnp.int32) * local + jnp.arange(local, dtype=jnp.int32)[None, :]
    scores = scores.at[0, 0].set(-1)
    scores = scores.at[shards - 1, local - 1].set(-1)
    ranking = jnp.argsort(jnp.argsort(scores, axis=1), axis=1).astype(jnp.int32)
    chosen = (ranking < full[:, None]).reshape(-1)
    orbital_ids = jnp.arange(shards * local, dtype=jnp.int32)
    keyed = jnp.where(chosen, orbital_ids, orbital_ids + shards * local)
    picked = jnp.sort(keyed)[:N]
    return jax.random.permutation(key_order, picked).astype(jnp.int32)


def with_ends(array, key, low, top_value):
    spot = [jax.random.randint(jax.random.fold_in(key, axis), (), 0, length) for axis, length in enumerate(array.shape)]
    main_axis = array.shape.index(max(array.shape))
    neighbour = spot[:main_axis] + [(spot[main_axis] + 1) % array.shape[main_axis]] + spot[main_axis + 1:]
    return array.at[tuple(spot)].set(low).at[tuple(neighbour)].set(top_value)


def block_levels(stream_key, dims, pieces, low, top_value):
    gain = 1.0
    for axis_at, shards_of in pieces:
        steps = jax.random.uniform(jax.random.fold_in(jax.random.fold_in(stream_key, 6), axis_at), (shards_of,), jnp.float32, low / len(pieces), top_value / len(pieces))
        gain = gain * jnp.repeat(jnp.exp(steps), dims[axis_at] // shards_of).reshape((-1,) + (1,) * (len(dims) - 1 - axis_at))
    return gain


def gaussian(stream_key, shape, deviation, most, cuts=(), held_as=jnp.bfloat16):
    result = jax.random.normal(stream_key, shape, jnp.float32) * deviation
    if len(cuts) > 0:
        result = block_levels(stream_key, shape, cuts, -0.22, 0.18) * result
    return jnp.clip(result, min=-most, max=most).astype(held_as)


def setup_inputs(seed: int = 0) -> dict:
    seeds = jax.random.split(jax.random.key(seed), 8)
    coefficients = gaussian(seeds[0], (CELLS, M), 1.0, 6.0, ((1, 8),))
    inverse = gaussian(seeds[1], (SAMPLES, N, N), (N * N) ** -0.5, 0.005859375, ((0, 4), (1, 8)))
    cell_index = with_ends(jax.random.randint(seeds[2], (SAMPLES, 3, N), 0, GRID), jax.random.fold_in(seeds[2], 1), 0, GRID - 1).astype(jnp.int32)
    fraction = jnp.clip(1.0 * jax.random.uniform(seeds[3], (SAMPLES, 3, N), jnp.float32) ** block_levels(seeds[3], (SAMPLES, 3, N), ((0, 4),), -0.2, 0.2), 0.0, 1.0)
    energies = gaussian(seeds[4], (SAMPLES,), 2.0, 8.0, ((0, 4),), jnp.float32)
    weights = jnp.clip(jnp.exp(math.log(2.0) - 1.3862944 * jax.random.uniform(seeds[5], (SAMPLES,), jnp.float32) ** block_levels(seeds[5], (SAMPLES,), ((0, 4),), -0.2, 0.2)), 0.5, 2.0)
    occupied = draw_occupied(jax.random.fold_in(seeds[7], 71), 0)
    return dict(coefficients=coefficients, inverse=inverse, cell_index=cell_index, fraction=fraction, energies=energies, weights=weights, occupied=occupied)


def spline_basis(frac):
    remain = 1.0 - frac
    square = frac * frac
    cubed = square * frac
    values = jnp.stack([remain * remain * remain, 3.0 * cubed - 6.0 * square + 4.0, -3.0 * cubed + 3.0 * square + 3.0 * frac + 1.0, cubed]) / 6.0
    curves = jnp.stack([remain, 3.0 * frac - 2.0, 1.0 - 3.0 * frac, frac])
    return values, curves


def evaluate(coefficients, cell_one, frac_one, edge):
    shifts = jnp.arange(4, dtype=jnp.int32)[:, None] - 1
    index_x = (cell_one[0][None, :] + shifts) % edge
    index_y = (cell_one[1][None, :] + shifts) % edge
    index_z = (cell_one[2][None, :] + shifts) % edge
    value_x, curve_x = spline_basis(frac_one[0])
    value_y, curve_y = spline_basis(frac_one[1])
    value_z, curve_z = spline_basis(frac_one[2])
    plane = (index_y[:, None, :] * edge + index_z[None, :, :]).reshape(16, -1)
    value_yz = (value_y[:, None, :] * value_z[None, :, :]).reshape(16, -1)
    curve_yz = (curve_y[:, None, :] * value_z[None, :, :] + value_y[:, None, :] * curve_z[None, :, :]).reshape(16, -1)
    electrons = cell_one.shape[1]
    orbital_sum = jnp.zeros((electrons, coefficients.shape[1]), jnp.float32)
    laplace_sum = jnp.zeros((electrons, coefficients.shape[1]), jnp.float32)
    for tap_x in range(4):
        tap_rows = index_x[tap_x][None, :] * (edge * edge) + plane
        tap_coef = jnp.take(coefficients, tap_rows, axis=0).astype(jnp.float32)
        weight_val = value_x[tap_x][None, :] * value_yz
        weight_lap = curve_x[tap_x][None, :] * value_yz + value_x[tap_x][None, :] * curve_yz
        orbital_sum = orbital_sum + jnp.einsum("kn,knw->nw", weight_val, tap_coef, precision=lax.Precision.HIGHEST)
        laplace_sum = laplace_sum + jnp.einsum("kn,knw->nw", weight_lap, tap_coef, precision=lax.Precision.HIGHEST)
    return orbital_sum.astype(jnp.bfloat16), laplace_sum.astype(jnp.bfloat16)


def wide_dot(left, right):
    return jnp.dot(left.astype(jnp.float32), right.astype(jnp.float32), precision=lax.Precision.HIGHEST)


def reference(coefficients, inverse, cell_index, fraction, energies, weights, occupied):
    def one_sample(running, items):
        inverse_one, cells_one, frac_one, energy, weight = items
        orbital_vals, laplace_vals = evaluate(coefficients, cells_one, frac_one, GRID)
        ratio = wide_dot(inverse_one, orbital_vals).astype(jnp.bfloat16)
        kinetic = wide_dot(inverse_one, laplace_vals)
        occupied_block = jnp.take(kinetic, occupied, axis=1).astype(jnp.bfloat16)
        coupled = wide_dot(occupied_block, ratio)
        sample_term = weight * (energy * ratio.astype(jnp.float32) - 0.5 * (kinetic - coupled))
        return running + sample_term, None

    initial = jnp.zeros((N, M), jnp.float32)
    gradient, unused = lax.scan(one_sample, initial, (inverse, cell_index, fraction, energies, weights))
    return gradient
```

```python
import functools
import jax
import jax.numpy as jnp
from jax import lax
from jax.experimental import pallas as pl
from jax.experimental.pallas import tpu as pltpu
from jax.sharding import PartitionSpec as P

GRID = 16
PLANE = GRID * GRID
MESH = pl.DeviceIdType.MESH
F32 = jnp.float32
BF16 = jnp.bfloat16
CONTRACT_LANES = (((1,), (1,)), ((), ()))


def spline_rows(frac):
    remain = 1.0 - frac
    square = frac * frac
    cubed = square * frac
    sixth = 1.0 / 6.0
    values = [
        remain * remain * remain * sixth,
        (3.0 * cubed - 6.0 * square + 4.0) * sixth,
        (-3.0 * cubed + 3.0 * square + 3.0 * frac + 1.0) * sixth,
        cubed * sixth,
    ]
    curves = [remain, 3.0 * frac - 2.0, 1.0 - 3.0 * frac, frac]
    return values, curves


def dense_tables(cell, frac):
    electrons = cell.shape[1]
    line = lax.broadcasted_iota(jnp.int32, (GRID, electrons), 0)
    values, curves = spline_rows(frac)
    value = jnp.zeros((GRID, electrons), F32)
    curve = jnp.zeros((GRID, electrons), F32)
    for tap in range(4):
        hit = line == ((cell + (GRID + tap - 1)) & (GRID - 1))
        value = value + jnp.where(hit, values[tap], 0.0)
        curve = curve + jnp.where(hit, curves[tap], 0.0)
    return value, curve


class LineGather:
    def __init__(self, buf, rows, chips, z, core, sems):
        self.buf, self.rows, self.chips, self.z, self.core = buf, rows, chips, z, core
        self.send, self.recv, self.sib_send, self.sib_recv = sems

    def block(self, owner):
        return self.buf.at[pl.ds(pl.multiple_of(owner * self.rows, self.rows), self.rows), :]

    def copy(self, owner, send, recv, target):
        return pltpu.make_async_remote_copy(
            src_ref=self.block(owner),
            dst_ref=self.block(owner),
            send_sem=send,
            recv_sem=recv,
            device_id={"orb": target},
            device_id_type=MESH,
        )

    def hop(self, way, k):
        sign = 1 - 2 * way
        chip = self.z - sign * k
        onto = self.z + sign
        copy = self.copy(
            chip * 2 + self.core, self.send.at[way, k], self.recv.at[way, k], onto * 2 + self.core
        )
        return copy, (chip >= 0) & (chip < self.chips) & (onto >= 0) & (onto < self.chips)

    def came(self, way, k):
        sign = 1 - 2 * way
        chip = self.z - sign * (k + 1)
        copy = self.copy(
            chip * 2 + self.core, self.send.at[way, k], self.recv.at[way, k], self.z * 2 + 1 - self.core
        )
        return chip, copy, (chip >= 0) & (chip < self.chips)

    def relay(self, chip, owner_core, slot):
        return self.copy(
            chip * 2 + owner_core, self.sib_send.at[slot], self.sib_recv.at[slot],
            self.z * 2 + 1 - self.core,
        )

    def step(self, k):
        if k == 0:
            for way in range(2):
                copy, sends = self.hop(way, 0)
                pl.when(sends)(copy.start)
            self.relay(self.z, self.core, 0).start()
            return
        for way in range(2):
            chip, arrived, comes = self.came(way, k - 1)
            pl.when(comes)(arrived.wait_recv)
            if k < self.chips - 1:
                copy, sends = self.hop(way, k)
                pl.when(sends)(copy.start)
            pl.when(comes)(self.relay(chip, self.core, 1 + 2 * (k - 1) + way).start)

    def sibling(self, k):
        if k == 0:
            self.relay(self.z, 1 - self.core, 0).wait_recv()
            return
        for way in range(2):
            chip, _, comes = self.came(way, k - 1)
            pl.when(comes)(self.relay(chip, 1 - self.core, 1 + 2 * (k - 1) + way).wait_recv)

    def drain(self):
        self.relay(self.z, self.core, 0).wait_send()
        for k in range(self.chips - 1):
            for way in range(2):
                copy, sends = self.hop(way, k)
                pl.when(sends)(copy.wait_send)
                chip, _, comes = self.came(way, k)
                pl.when(comes)(self.relay(chip, self.core, 1 + 2 * k + way).wait_send)


def kernel(
    dims,
    coef_hbm, inv_ref, cell_ref, frac_ref, energy_ref, weight_ref, occ_ref,
    out_ref,
    coef, inv_all, sel_all, xt, yzv, yzl, w_scr, phi, lap, ratio, rsel, total, send_buf, recv_buf,
    coef_sem, own_sem, i_send, i_recv, i_sib_send, i_sib_recv,
    s_send, s_recv, s_sib_send, s_sib_recv, g_send, g_recv,
):
    walkers, orbs, capacity, block = dims
    chips = orbs // 2
    electrons = cell_ref.shape[2]
    width = coef.shape[1]
    inv_rows = inv_ref.shape[1]
    out_rows = out_ref.shape[0]
    me_walk = lax.axis_index("walk")
    me_orb = lax.axis_index("orb")
    z = me_orb // 2
    core = me_orb % 2

    load = pltpu.make_async_copy(coef_hbm, coef, coef_sem)
    load.start()
    gather_inv = LineGather(inv_all, inv_rows, chips, z, core, (i_send, i_recv, i_sib_send, i_sib_recv))
    gather_sel = LineGather(sel_all, capacity, chips, z, core, (s_send, s_recv, s_sib_send, s_sib_recv))
    own = pltpu.make_async_copy(inv_ref.at[0], gather_inv.block(me_orb), own_sem)
    own.start()

    barrier = pltpu.get_barrier_semaphore()
    pl.semaphore_signal(barrier, inc=1, device_id={"orb": z * 2 + 1 - core}, device_id_type=MESH)
    for step in range(1, walkers):
        peer = lax.rem(me_walk + step, walkers)
        pl.semaphore_signal(barrier, inc=1, device_id={"walk": peer}, device_id_type=MESH)

    @pl.when(z > 0)
    def _():
        pl.semaphore_signal(barrier, inc=1, device_id={"orb": me_orb - 2}, device_id_type=MESH)

    @pl.when(z < chips - 1)
    def _():
        pl.semaphore_signal(barrier, inc=1, device_id={"orb": me_orb + 2}, device_id_type=MESH)

    neighbours = jnp.where(z > 0, 1, 0) + jnp.where(z < chips - 1, 1, 0)
    pl.semaphore_wait(barrier, walkers + neighbours)

    own.wait()
    gather_inv.step(0)

    xv, xc = dense_tables(cell_ref[0, 0:1, :], frac_ref[0, 0:1, :])
    yv, yc = dense_tables(cell_ref[0, 1:2, :], frac_ref[0, 1:2, :])
    zv, zc = dense_tables(cell_ref[0, 2:3, :], frac_ref[0, 2:3, :])
    xt[0:GRID, :] = xv
    xt[GRID:2 * GRID, :] = xc
    xt[2 * GRID:, :] = jnp.zeros((xt.shape[0] - 2 * GRID, electrons), F32)
    for y in range(GRID):
        at = slice(y * GRID, (y + 1) * GRID)
        yzv[at, :] = yv[y:y + 1, :] * zv
        yzl[at, :] = yc[y:y + 1, :] * zv + yv[y:y + 1, :] * zc

    occ = occ_ref[...]
    owner = occ // width
    ones = lax.broadcasted_iota(jnp.int32, (orbs, electrons), 0) == owner
    before = (
        lax.broadcasted_iota(jnp.int32, (electrons, electrons), 0)
        < lax.broadcasted_iota(jnp.int32, (electrons, electrons), 1)
    )
    counts = jnp.dot(
        jnp.where(ones, 1.0, 0.0).astype(BF16), jnp.where(before, 1.0, 0.0).astype(BF16),
        preferred_element_type=F32,
    )
    rank = jnp.sum(jnp.where(ones, counts, 0.0), axis=0, keepdims=True)
    slot = owner * capacity + rank.astype(jnp.int32)
    local = occ - me_orb * width
    row_hit = lax.broadcasted_iota(jnp.int32, (width, electrons), 0) == local
    my_slot = slot - me_orb * capacity
    slot_hit = (lax.broadcasted_iota(jnp.int32, (capacity, electrons), 0) == my_slot)
    picker = lax.dot_general(
        jnp.where(slot_hit, 1.0, 0.0).astype(BF16), jnp.where(row_hit, 1.0, 0.0).astype(BF16),
        CONTRACT_LANES, preferred_element_type=F32,
    ).astype(BF16)

    load.wait()

    def evaluate(at, carry):
        cols = pl.ds(pl.multiple_of(at * block, block), block)
        x_tab = jnp.transpose(xt[:, cols])
        plane_v = jnp.transpose(yzv[:, cols])
        plane_l = jnp.transpose(yzl[:, cols])
        for x in range(GRID):
            val = x_tab[:, x:x + 1]
            cur = x_tab[:, GRID + x:GRID + x + 1]
            lanes = slice(x * PLANE, (x + 1) * PLANE)
            w_scr[0:block, lanes] = (val * plane_v).astype(BF16)
            w_scr[block:, lanes] = (cur * plane_v + val * plane_l).astype(BF16)
        both = jnp.dot(w_scr[...], coef[...], preferred_element_type=F32)
        phi[:, cols] = jnp.transpose(both[0:block]).astype(BF16)
        lap[:, cols] = jnp.transpose(both[block:]).astype(BF16)
        return carry

    trips = electrons // block
    lax.fori_loop(0, trips // 2, evaluate, 0)
    gather_inv.step(1)
    lax.fori_loop(trips // 2, trips, evaluate, 0)
    mine = pl.ds(pl.multiple_of(me_orb * capacity, capacity), capacity)
    sel_all[mine, :] = jnp.dot(picker, lap[...], preferred_element_type=F32).astype(BF16)
    gather_sel.step(0)
    for k in range(2, chips):
        gather_inv.step(k)
    for k in range(chips):
        gather_inv.sibling(k)
    if chips > 1:
        pass

    def ratio_block(chip, carry):
        rows = pl.ds(pl.multiple_of(chip * 2 * inv_rows, 2 * inv_rows), 2 * inv_rows)
        ratio[:, rows] = lax.dot_general(
            phi[...], inv_all[rows, :], CONTRACT_LANES, preferred_element_type=F32
        ).astype(BF16)
        return carry

    lax.fori_loop(0, chips, ratio_block, 0)

    pair = 2 * capacity

    def pick_block(chip, carry):
        hit = lax.broadcasted_iota(jnp.int32, (pair, electrons), 0) + chip * pair == slot
        rsel[pl.ds(chip, 1)] = lax.dot_general(
            ratio[...], jnp.where(hit, 1.0, 0.0).astype(BF16), CONTRACT_LANES,
            preferred_element_type=F32,
        ).astype(BF16)[None]
        return carry

    lax.fori_loop(0, chips, pick_block, 0)

    energy = energy_ref[0]
    weight = weight_ref[0]
    total[...] = (weight * energy) * phi[...].astype(F32) - (0.5 * weight) * lap[...].astype(F32)

    def couple(chip):
        rows = pl.ds(pl.multiple_of(chip * pair, pair), pair)
        total[...] += (0.5 * weight) * jnp.dot(
            rsel[pl.ds(chip, 1)][0], sel_all[rows, :], preferred_element_type=F32
        )

    gather_sel.sibling(0)
    couple(z)
    for k in range(1, chips):
        gather_sel.step(k)
        gather_sel.sibling(k)
        if k < chips - 1 or chips <= 1:
            pass
        for way in range(2):
            chip, _, comes = gather_sel.came(way, k - 1)
            pl.when(comes)(functools.partial(couple, chip))

    phi[...] = total[...].astype(BF16)

    def product(peer):
        rows = pl.ds(pl.multiple_of(peer * out_rows, out_rows), out_rows)
        return lax.dot_general(
            inv_all[rows, :], phi[...], CONTRACT_LANES, preferred_element_type=F32
        )

    copies = []
    for step in range(1, walkers):
        peer = lax.rem(me_walk + walkers - step, walkers)
        send_buf[step - 1] = product(peer).astype(BF16)
        copy = pltpu.make_async_remote_copy(
            src_ref=send_buf.at[step - 1],
            dst_ref=recv_buf.at[step - 1],
            send_sem=g_send.at[step - 1],
            recv_sem=g_recv.at[step - 1],
            device_id={"walk": peer},
            device_id_type=MESH,
        )
        copy.start()
        copies.append(copy)
    out_ref[...] = product(me_walk)
    for step, copy in enumerate(copies):
        copy.wait_recv()
        out_ref[...] += recv_buf[step].astype(F32)
    for copy in copies:
        copy.wait_send()
    gather_inv.drain()
    gather_sel.drain()


def body(coefficients, inverse, cell_index, fraction, energies, weights, occupied):
    walkers = lax.axis_size("walk")
    orbs = lax.axis_size("orb")
    chips = orbs // 2
    cells, width = coefficients.shape
    inv_rows = inverse.shape[1]
    electrons = inverse.shape[2]
    capacity = 3 * electrons // (2 * orbs)
    block = min(256, electrons)
    out_rows = electrons // walkers
    dims = (walkers, orbs, capacity, block)
    dma = pltpu.SemaphoreType.DMA
    hops = (2, max(chips - 1, 1))
    relays = (1 + 2 * (chips - 1),)
    vmem = pl.BlockSpec(memory_space=pltpu.VMEM)
    smem = pl.BlockSpec(memory_space=pltpu.SMEM)
    return pl.pallas_call(
        functools.partial(kernel, dims),
        out_shape=jax.ShapeDtypeStruct((out_rows, width), F32),
        in_specs=[pl.BlockSpec(memory_space=pl.ANY), vmem, vmem, vmem, smem, smem, vmem],
        out_specs=vmem,
        scratch_shapes=[
            pltpu.VMEM((cells, width), BF16),
            pltpu.VMEM((electrons, electrons), BF16),
            pltpu.VMEM((orbs * capacity, electrons), BF16),
            pltpu.VMEM((128, electrons), F32),
            pltpu.VMEM((PLANE, electrons), F32),
            pltpu.VMEM((PLANE, electrons), F32),
            pltpu.VMEM((2 * block, cells), BF16),
            pltpu.VMEM((width, electrons), BF16),
            pltpu.VMEM((width, electrons), BF16),
            pltpu.VMEM((width, electrons), BF16),
            pltpu.VMEM((chips, width, 2 * capacity), BF16),
            pltpu.VMEM((width, electrons), F32),
            pltpu.VMEM((max(walkers - 1, 1), out_rows, width), BF16),
            pltpu.VMEM((max(walkers - 1, 1), out_rows, width), BF16),
            dma, dma,
            dma(hops), dma(hops), dma(relays), dma(relays),
            dma(hops), dma(hops), dma(relays), dma(relays),
            dma((max(walkers - 1, 1),)), dma((max(walkers - 1, 1),)),
        ],
        compiler_params=pltpu.CompilerParams(
            collective_id=0, has_side_effects=True, vmem_limit_bytes=60 * 1024 * 1024
        ),
        name="gradient",
    )(coefficients, inverse, cell_index, fraction, energies, weights, occupied.reshape(1, electrons))


def solution(mesh):
    in_specs = (
        P(None, "orb"),
        P("walk", "orb", None),
        P("walk", None, None),
        P("walk", None, None),
        P("walk"),
        P("walk"),
        P(),
    )
    out_specs = P("walk", "orb")
    return jax.shard_map(body, mesh=mesh, in_specs=in_specs, out_specs=out_specs, check_vma=False)
```

```python
import functools
import jax
import jax.numpy as jnp
from jax import lax
from jax.experimental import pallas as pl
from jax.experimental.pallas import tpu as pltpu
from jax.sharding import PartitionSpec as P

GRID = 16
PLANE = GRID * GRID
MESH = pl.DeviceIdType.MESH
F32 = jnp.float32
BF16 = jnp.bfloat16
CONTRACT_LANES = (((1,), (1,)), ((), ()))


def spline_rows(frac):
    remain = 1.0 - frac
    square = frac * frac
    cubed = square * frac
    sixth = 1.0 / 6.0
    values = [
        remain * remain * remain * sixth,
        (3.0 * cubed - 6.0 * square + 4.0) * sixth,
        (-3.0 * cubed + 3.0 * square + 3.0 * frac + 1.0) * sixth,
        cubed * sixth,
    ]
    curves = [remain, 3.0 * frac - 2.0, 1.0 - 3.0 * frac, frac]
    return values, curves


def dense_tables(cell, frac):
    electrons = cell.shape[1]
    line = lax.broadcasted_iota(jnp.int32, (GRID, electrons), 0)
    values, curves = spline_rows(frac)
    value = jnp.zeros((GRID, electrons), F32)
    curve = jnp.zeros((GRID, electrons), F32)
    for tap in range(4):
        hit = line == ((cell + (GRID + tap - 1)) & (GRID - 1))
        value = value + jnp.where(hit, values[tap], 0.0)
        curve = curve + jnp.where(hit, curves[tap], 0.0)
    return value, curve


class LineGather:
    def __init__(self, buf, rows, chips, z, core, sems):
        self.buf, self.rows, self.chips, self.z, self.core = buf, rows, chips, z, core
        self.send, self.recv, self.sib_send, self.sib_recv = sems

    def block(self, owner):
        return self.buf.at[pl.ds(pl.multiple_of(owner * self.rows, self.rows), self.rows), :]

    def copy(self, owner, send, recv, target):
        return pltpu.make_async_remote_copy(
            src_ref=self.block(owner),
            dst_ref=self.block(owner),
            send_sem=send,
            recv_sem=recv,
            device_id={"orb": target},
            device_id_type=MESH,
        )

    def hop(self, way, k):
        sign = 1 - 2 * way
        chip = self.z - sign * k
        onto = self.z + sign
        copy = self.copy(
            chip * 2 + self.core, self.send.at[way, k], self.recv.at[way, k], onto * 2 + self.core
        )
        return copy, (chip >= 0) & (chip < self.chips) & (onto >= 0) & (onto < self.chips)

    def came(self, way, k):
        sign = 1 - 2 * way
        chip = self.z - sign * (k + 1)
        copy = self.copy(
            chip * 2 + self.core, self.send.at[way, k], self.recv.at[way, k], self.z * 2 + 1 - self.core
        )
        return chip, copy, (chip >= 0) & (chip < self.chips)

    def relay(self, chip, owner_core, slot):
        return self.copy(
            chip * 2 + owner_core, self.sib_send.at[slot], self.sib_recv.at[slot],
            self.z * 2 + 1 - self.core,
        )

    def step(self, k):
        if k == 0:
            for way in range(2):
                copy, sends = self.hop(way, 0)
                pl.when(sends)(copy.start)
            self.relay(self.z, self.core, 0).start()
            return
        for way in range(2):
            chip, arrived, comes = self.came(way, k - 1)
            pl.when(comes)(arrived.wait_recv)
            if k < self.chips - 1:
                copy, sends = self.hop(way, k)
                pl.when(sends)(copy.start)
            pl.when(comes)(self.relay(chip, self.core, 1 + 2 * (k - 1) + way).start)

    def sibling(self, k):
        if k == 0:
            self.relay(self.z, 1 - self.core, 0).wait_recv()
            return
        for way in range(2):
            chip, _, comes = self.came(way, k - 1)
            pl.when(comes)(self.relay(chip, 1 - self.core, 1 + 2 * (k - 1) + way).wait_recv)

    def drain(self):
        self.relay(self.z, self.core, 0).wait_send()
        for k in range(self.chips - 1):
            for way in range(2):
                copy, sends = self.hop(way, k)
                pl.when(sends)(copy.wait_send)
                chip, _, comes = self.came(way, k)
                pl.when(comes)(self.relay(chip, self.core, 1 + 2 * k + way).wait_send)


def kernel(
    dims,
    coef_hbm, inv_ref, cell_ref, frac_ref, energy_ref, weight_ref, occ_ref,
    out_ref,
    coef, inv_all, sel_all, xt, yzv, yzl, w_scr, phi, lap, ratio, rsel, total, send_buf, recv_buf,
    coef_sem, own_sem, i_send, i_recv, i_sib_send, i_sib_recv,
    s_send, s_recv, s_sib_send, s_sib_recv, g_send, g_recv,
):
    walkers, orbs, capacity, block = dims
    chips = orbs // 2
    electrons = cell_ref.shape[2]
    width = coef.shape[1]
    inv_rows = inv_ref.shape[1]
    out_rows = out_ref.shape[0]
    me_walk = lax.axis_index("walk")
    me_orb = lax.axis_index("orb")
    z = me_orb // 2
    core = me_orb % 2

    load = pltpu.make_async_copy(coef_hbm, coef, coef_sem)
    load.start()
    gather_inv = LineGather(inv_all, inv_rows, chips, z, core, (i_send, i_recv, i_sib_send, i_sib_recv))
    gather_sel = LineGather(sel_all, capacity, chips, z, core, (s_send, s_recv, s_sib_send, s_sib_recv))
    own = pltpu.make_async_copy(inv_ref.at[0], gather_inv.block(me_orb), own_sem)
    own.start()

    barrier = pltpu.get_barrier_semaphore()
    pl.semaphore_signal(barrier, inc=1, device_id={"orb": z * 2 + 1 - core}, device_id_type=MESH)
    for step in range(1, walkers):
        peer = lax.rem(me_walk + step, walkers)
        pl.semaphore_signal(barrier, inc=1, device_id={"walk": peer}, device_id_type=MESH)

    @pl.when(z > 0)
    def _():
        pl.semaphore_signal(barrier, inc=1, device_id={"orb": me_orb - 2}, device_id_type=MESH)

    @pl.when(z < chips - 1)
    def _():
        pl.semaphore_signal(barrier, inc=1, device_id={"orb": me_orb + 2}, device_id_type=MESH)

    neighbours = jnp.where(z > 0, 1, 0) + jnp.where(z < chips - 1, 1, 0)
    pl.semaphore_wait(barrier, walkers + neighbours)

    own.wait()
    gather_inv.step(0)

    xv, xc = dense_tables(cell_ref[0, 0:1, :], frac_ref[0, 0:1, :])
    yv, yc = dense_tables(cell_ref[0, 1:2, :], frac_ref[0, 1:2, :])
    zv, zc = dense_tables(cell_ref[0, 2:3, :], frac_ref[0, 2:3, :])
    xt[0:GRID, :] = xv
    xt[GRID:2 * GRID, :] = xc
    xt[2 * GRID:, :] = jnp.zeros((xt.shape[0] - 2 * GRID, electrons), F32)
    for y in range(GRID):
        at = slice(y * GRID, (y + 1) * GRID)
        yzv[at, :] = yv[y:y + 1, :] * zv
        yzl[at, :] = yc[y:y + 1, :] * zv + yv[y:y + 1, :] * zc

    occ = occ_ref[...]
    owner = occ // width
    ones = lax.broadcasted_iota(jnp.int32, (orbs, electrons), 0) == owner
    before = (
        lax.broadcasted_iota(jnp.int32, (electrons, electrons), 0)
        < lax.broadcasted_iota(jnp.int32, (electrons, electrons), 1)
    )
    counts = jnp.dot(
        jnp.where(ones, 1.0, 0.0).astype(BF16), jnp.where(before, 1.0, 0.0).astype(BF16),
        preferred_element_type=F32,
    )
    rank = jnp.sum(jnp.where(ones, counts, 0.0), axis=0, keepdims=True)
    slot = owner * capacity + rank.astype(jnp.int32)
    local = occ - me_orb * width
    row_hit = lax.broadcasted_iota(jnp.int32, (width, electrons), 0) == local
    my_slot = slot - me_orb * capacity
    slot_hit = (lax.broadcasted_iota(jnp.int32, (capacity, electrons), 0) == my_slot)
    picker = lax.dot_general(
        jnp.where(slot_hit, 1.0, 0.0).astype(BF16), jnp.where(row_hit, 1.0, 0.0).astype(BF16),
        CONTRACT_LANES, preferred_element_type=F32,
    ).astype(BF16)

    load.wait()

    trips = electrons // block
    within = max(1, min(chips, trips - 1))

    def evaluate(at, carry):
        for k in range(1, within):
            pl.when(at == k + 1)(functools.partial(gather_inv.step, k))
        cols = pl.ds(pl.multiple_of(at * block, block), block)
        x_tab = jnp.transpose(xt[:, cols])
        plane_v = jnp.transpose(yzv[:, cols])
        plane_l = jnp.transpose(yzl[:, cols])
        for x in range(GRID):
            val = x_tab[:, x:x + 1]
            cur = x_tab[:, GRID + x:GRID + x + 1]
            lanes = slice(x * PLANE, (x + 1) * PLANE)
            w_scr[0:block, lanes] = (val * plane_v).astype(BF16)
            w_scr[block:, lanes] = (cur * plane_v + val * plane_l).astype(BF16)
        both = jnp.dot(w_scr[...], coef[...], preferred_element_type=F32)
        phi[:, cols] = jnp.transpose(both[0:block]).astype(BF16)
        lap[:, cols] = jnp.transpose(both[block:]).astype(BF16)
        return carry

    lax.fori_loop(0, trips, evaluate, 0)
    mine = pl.ds(pl.multiple_of(me_orb * capacity, capacity), capacity)
    sel_all[mine, :] = jnp.dot(picker, lap[...], preferred_element_type=F32).astype(BF16)
    gather_sel.step(0)
    for k in range(within, chips):
        gather_inv.step(k)
    for k in range(chips):
        gather_inv.sibling(k)

    def ratio_block(chip, carry):
        rows = pl.ds(pl.multiple_of(chip * 2 * inv_rows, 2 * inv_rows), 2 * inv_rows)
        ratio[:, rows] = lax.dot_general(
            phi[...], inv_all[rows, :], CONTRACT_LANES, preferred_element_type=F32
        ).astype(BF16)
        return carry

    lax.fori_loop(0, chips, ratio_block, 0)
    if chips > 1:
        gather_sel.step(1)

    pair = 2 * capacity

    def pick_block(chip, carry):
        hit = lax.broadcasted_iota(jnp.int32, (pair, electrons), 0) + chip * pair == slot
        rsel[pl.ds(chip, 1)] = lax.dot_general(
            ratio[...], jnp.where(hit, 1.0, 0.0).astype(BF16), CONTRACT_LANES,
            preferred_element_type=F32,
        ).astype(BF16)[None]
        return carry

    lax.fori_loop(0, chips, pick_block, 0)

    energy = energy_ref[0]
    weight = weight_ref[0]
    total[...] = (weight * energy) * phi[...].astype(F32) - (0.5 * weight) * lap[...].astype(F32)

    def couple(chip):
        rows = pl.ds(pl.multiple_of(chip * pair, pair), pair)
        total[...] += (0.5 * weight) * jnp.dot(
            rsel[pl.ds(chip, 1)][0], sel_all[rows, :], preferred_element_type=F32
        )

    gather_sel.sibling(0)
    couple(z)
    for k in range(1, chips):
        if k > 1:
            gather_sel.step(k)
        gather_sel.sibling(k)
        for way in range(2):
            chip, _, comes = gather_sel.came(way, k - 1)
            pl.when(comes)(functools.partial(couple, chip))

    phi[...] = total[...].astype(BF16)

    def product(peer):
        rows = pl.ds(pl.multiple_of(peer * out_rows, out_rows), out_rows)
        return lax.dot_general(
            inv_all[rows, :], phi[...], CONTRACT_LANES, preferred_element_type=F32
        )

    copies = []
    for step in range(1, walkers):
        peer = lax.rem(me_walk + walkers - step, walkers)
        send_buf[step - 1] = product(peer).astype(BF16)
        copy = pltpu.make_async_remote_copy(
            src_ref=send_buf.at[step - 1],
            dst_ref=recv_buf.at[step - 1],
            send_sem=g_send.at[step - 1],
            recv_sem=g_recv.at[step - 1],
            device_id={"walk": peer},
            device_id_type=MESH,
        )
        copy.start()
        copies.append(copy)
    out_ref[...] = product(me_walk)
    for step, copy in enumerate(copies):
        copy.wait_recv()
        out_ref[...] += recv_buf[step].astype(F32)
    for copy in copies:
        copy.wait_send()
    gather_inv.drain()
    gather_sel.drain()


def body(coefficients, inverse, cell_index, fraction, energies, weights, occupied):
    walkers = lax.axis_size("walk")
    orbs = lax.axis_size("orb")
    chips = orbs // 2
    cells, width = coefficients.shape
    inv_rows = inverse.shape[1]
    electrons = inverse.shape[2]
    capacity = 3 * electrons // (2 * orbs)
    block = min(256, electrons)
    out_rows = electrons // walkers
    dims = (walkers, orbs, capacity, block)
    dma = pltpu.SemaphoreType.DMA
    hops = (2, max(chips - 1, 1))
    relays = (1 + 2 * (chips - 1),)
    vmem = pl.BlockSpec(memory_space=pltpu.VMEM)
    smem = pl.BlockSpec(memory_space=pltpu.SMEM)
    return pl.pallas_call(
        functools.partial(kernel, dims),
        out_shape=jax.ShapeDtypeStruct((out_rows, width), F32),
        in_specs=[pl.BlockSpec(memory_space=pl.ANY), vmem, vmem, vmem, smem, smem, vmem],
        out_specs=vmem,
        scratch_shapes=[
            pltpu.VMEM((cells, width), BF16),
            pltpu.VMEM((electrons, electrons), BF16),
            pltpu.VMEM((orbs * capacity, electrons), BF16),
            pltpu.VMEM((128, electrons), F32),
            pltpu.VMEM((PLANE, electrons), F32),
            pltpu.VMEM((PLANE, electrons), F32),
            pltpu.VMEM((2 * block, cells), BF16),
            pltpu.VMEM((width, electrons), BF16),
            pltpu.VMEM((width, electrons), BF16),
            pltpu.VMEM((width, electrons), BF16),
            pltpu.VMEM((chips, width, 2 * capacity), BF16),
            pltpu.VMEM((width, electrons), F32),
            pltpu.VMEM((max(walkers - 1, 1), out_rows, width), BF16),
            pltpu.VMEM((max(walkers - 1, 1), out_rows, width), BF16),
            dma, dma,
            dma(hops), dma(hops), dma(relays), dma(relays),
            dma(hops), dma(hops), dma(relays), dma(relays),
            dma((max(walkers - 1, 1),)), dma((max(walkers - 1, 1),)),
        ],
        compiler_params=pltpu.CompilerParams(
            collective_id=0, has_side_effects=True, vmem_limit_bytes=60 * 1024 * 1024
        ),
        name="gradient",
    )(coefficients, inverse, cell_index, fraction, energies, weights, occupied.reshape(1, electrons))


def solution(mesh):
    in_specs = (
        P(None, "orb"),
        P("walk", "orb", None),
        P("walk", None, None),
        P("walk", None, None),
        P("walk"),
        P("walk"),
        P(),
    )
    out_specs = P("walk", "orb")
    return jax.shard_map(body, mesh=mesh, in_specs=in_specs, out_specs=out_specs, check_vma=False)
```
